32 devices in a mesh: cp: 8 (over y, x, core), tp: 4 (over z).
Axes of the slice: x: 2, y: 2, z: 4, core: 2. Of those that a mesh axis runs over, the one named last changes fastest.
Arguments:
- hidden: bfloat16 [2048, 4096], P('cp', 'tp'), may hold values from -120 to 120
- query_weight: bfloat16 [4096, 4096], P(None, 'tp'), may hold values from -0.1875 to 0.1875
- key_matrix: bfloat16 [4096, 512], P(None, 'tp'), may hold values from -0.09375 to 0.09375
- value_matrix: bfloat16 [4096, 512], P(None, 'tp'), may hold values from -0.09375 to 0.09375
- output_weight: bfloat16 [4096, 4096], P('tp'), may hold values from -0.1875 to 0.1875
- document_bounds: int32 [9], replicated, may hold values from 0 to 2048, as said below
- block_owner: int32 [16], replicated, may hold values from 0 to 7, as said below
Outputs:
- attended: bfloat16 [2048, 4096], P('cp', 'tp')
The draws below stay inside these ranges and needn't reach their ends.
Inputs may be any that keep to these rules, and one draw needn't show every extreme that they name: document_bounds[0] = 0, document_bounds[8] = 2048, strictly rising; document i holds the tokens from document_bounds[i] to document_bounds[i + 1] - 1. `block_owner`: every index of cp is named by exactly 2 blocks.
All inputs are finite; a program needn't handle non-finite values.
Results may differ from the reference program's by a relative error of at most 0.012.
The reference program's roundings to bfloat16 on the way (of `queries`, `values`, `heads_out` and `projected`) count: a program that leaves them out, or rounds other values in their place, can miss the bound.
Values may be sent and summed in bfloat16 or wider, within the bound.
A program may use at most 128 MiB of HBM per device.

```python
import math
import jax
import jax.numpy as jnp
from jax import lax

MODEL_WIDTH = 4096
QUERY_HEADS = 32
KEY_VALUE_HEADS = 4
HEAD_WIDTH = 128
BLOCK = 128
DOCS = 8
TOK_DEV = 256
PACKED_TOKENS = 2048
NBLK = 16


def draw_hidden(key, part):
    drawn = jax.random.normal(key, (PACKED_TOKENS, MODEL_WIDTH), jnp.float32)
    return jnp.clip(drawn, -6.0, 6.0).astype(jnp.bfloat16)


def draw_document_bounds(key, part):
    cut_points = jax.random.permutation(jax.random.fold_in(key, 21), PACKED_TOKENS - 1)[:DOCS - 1] + 1
    inner_cuts = jnp.sort(cut_points).astype(jnp.int32)
    return jnp.concatenate([jnp.zeros((1,), jnp.int32), inner_cuts, jnp.full((1,), PACKED_TOKENS, jnp.int32)])


def draw_block_owner(key, part):
    shuffled = jax.random.permutation(jax.random.fold_in(key, 31), NBLK)
    return (shuffled // (TOK_DEV // BLOCK)).astype(jnp.int32)


def steps_of(key, shape, pieces, low, largest):
    factor_of, own = 1.0, jax.random.fold_in(key, 6)
    for position, blocks in pieces:
        draws = jnp.exp(jax.random.uniform(jax.random.fold_in(own, position), (blocks,), jnp.float32, low / len(pieces), largest / len(pieces)))
        factor_of = factor_of * jnp.repeat(draws, shape[position] // blocks).reshape([-1 if axis == position else 1 for axis in range(len(shape))])
    return factor_of


def normal_values(own_key, shape, scale, most, shards=(), held_as=jnp.bfloat16):
    values = jax.random.normal(own_key, shape, jnp.float32) * scale
    if len(shards) > 0:
        values = steps_of(own_key, shape, shards, -0.22, 0.18) * values
    return jnp.clip(values, min=-most, max=most).astype(held_as)


def setup_inputs(seed: int = 0) -> dict:
    streams_of = jax.random.split(jax.random.key(seed), 8)
    return {
        "hidden": draw_hidden(jax.random.fold_in(streams_of[7], 71), 0),
        "query_weight": normal_values(streams_of[1], (MODEL_WIDTH, QUERY_HEADS * HEAD_WIDTH), (MODEL_WIDTH // 4) ** -0.5, 0.1875, ((1, 4),)),
        "key_matrix": normal_values(streams_of[2], (MODEL_WIDTH, KEY_VALUE_HEADS * HEAD_WIDTH), MODEL_WIDTH ** -0.5, 0.09375, ((1, 4),)),
        "value_matrix": normal_values(streams_of[3], (MODEL_WIDTH, KEY_VALUE_HEADS * HEAD_WIDTH), MODEL_WIDTH ** -0.5, 0.09375, ((1, 4),)),
        "output_weight": normal_values(streams_of[4], (QUERY_HEADS * HEAD_WIDTH, MODEL_WIDTH), (QUERY_HEADS * HEAD_WIDTH // 4) ** -0.5, 0.1875, ((0, 4),)),
        "document_bounds": draw_document_bounds(jax.random.fold_in(streams_of[7], 71), 0),
        "block_owner": draw_block_owner(jax.random.fold_in(streams_of[7], 71), 0),
    }


rope_theta = 500000.0
rope_factor = 8.0
rope_context = 8192.0
masked_score = -1e+30

def rope_inverse(head_size):
    halves = jnp.arange(head_size // 2, dtype=jnp.float32)
    inverse = 1.0 / rope_theta ** (2.0 * halves / head_size)
    wavelength = 2.0 * math.pi / inverse
    smooth = (rope_context / wavelength - 1.0) / 3.0
    blended = (1.0 - smooth) * inverse / rope_factor + smooth * inverse
    longer = jnp.where(wavelength > rope_context, inverse / rope_factor, blended)
    return jnp.where(wavelength < rope_context / 4.0, inverse, longer)

def document_of(tokens, bounds):
    inner_bounds = bounds[1:-1]
    return lax.optimization_barrier(jnp.sum((tokens[:, None] >= inner_bounds[None, :]).astype(jnp.int32), axis=1))

def position_of(tokens, bounds):
    starts = bounds[:-1]
    document_start = lax.optimization_barrier(jnp.max(jnp.where(starts[None, :] <= tokens[:, None], starts[None, :], 0), axis=1))
    return tokens - document_start

def rotate(raw_rows, tokens, bounds, head_size):
    row_count = raw_rows.shape[0]
    head_count = raw_rows.shape[1] // head_size
    angles = position_of(tokens, bounds).astype(jnp.float32)[:, None] * rope_inverse(head_size)[None, :]
    cosine = jnp.cos(angles)[:, None, :]
    sine_table = jnp.sin(angles)[:, None, :]
    heads_view = raw_rows.reshape(row_count, head_count, head_size)
    front_half = heads_view[:, :, :head_size // 2]
    back_half = heads_view[:, :, head_size // 2:]
    turned = jnp.concatenate([front_half * cosine - back_half * sine_table, back_half * cosine + front_half * sine_table], axis=2)
    return turned.reshape(row_count, head_count * head_size).astype(jnp.bfloat16)

def owner_order(block_owner, per_device):
    block_count = block_owner.shape[0]
    blocks = jnp.arange(block_count, dtype=jnp.int32)
    same_owner = block_owner[:, None] == block_owner[None, :]
    earlier = blocks[None, :] < blocks[:, None]
    owner_rank = lax.optimization_barrier(jnp.sum((same_owner & earlier).astype(jnp.int32), axis=1))
    target = block_owner * per_device + owner_rank
    return lax.optimization_barrier(jnp.sum(jnp.where(target[None, :] == blocks[:, None], blocks[None, :], 0), axis=1)).astype(jnp.int32)

def reference(hidden, query_weight, key_matrix, value_matrix, output_weight, document_bounds, block_owner):
    tokens = jnp.arange(PACKED_TOKENS, dtype=jnp.int32)
    query_raw = jnp.dot(hidden, query_weight, preferred_element_type=jnp.float32)
    key_raw = jnp.dot(hidden, key_matrix, preferred_element_type=jnp.float32)
    value_raw = jnp.dot(hidden, value_matrix, preferred_element_type=jnp.float32)
    queries = rotate(query_raw, tokens, document_bounds, HEAD_WIDTH)
    key_rows = rotate(key_raw, tokens, document_bounds, HEAD_WIDTH)
    value_rows = value_raw.astype(jnp.bfloat16)
    documents = document_of(tokens, document_bounds)
    query_heads = queries.reshape(PACKED_TOKENS, QUERY_HEADS, HEAD_WIDTH).transpose(1, 0, 2)
    per_head_keys = key_rows.reshape(PACKED_TOKENS, KEY_VALUE_HEADS, HEAD_WIDTH).transpose(1, 0, 2)
    per_head_values = value_rows.reshape(PACKED_TOKENS, KEY_VALUE_HEADS, HEAD_WIDTH).transpose(1, 0, 2)
    query_group_width = QUERY_HEADS // KEY_VALUE_HEADS
    query_block = math.gcd(PACKED_TOKENS, 1024)
    score_scale = 1.0 / math.sqrt(HEAD_WIDTH)

    def one_head(head_index):
        head_queries = query_heads[head_index]
        head_keys = per_head_keys[head_index // query_group_width]
        head_values = per_head_values[head_index // query_group_width]

        def one_block(block_index):
            first_row = block_index * query_block
            block_queries = lax.dynamic_slice_in_dim(head_queries, first_row, query_block, 0)
            block_tokens = first_row + jnp.arange(query_block, dtype=jnp.int32)
            block_documents = lax.dynamic_slice_in_dim(documents, first_row, query_block, 0)
            allowed = (block_documents[:, None] == documents[None, :]) & (tokens[None, :] <= block_tokens[:, None])
            scores = jnp.dot(block_queries, head_keys.T, preferred_element_type=jnp.float32) * score_scale
            scores = jnp.where(allowed, scores, masked_score)
            row_max = lax.optimization_barrier(jnp.max(scores, axis=1, keepdims=True))
            weights = jnp.where(allowed, jnp.exp(scores - row_max), 0.0)
            totals = lax.optimization_barrier(jnp.sum(weights, axis=1, keepdims=True))
            mixed_rows = jnp.dot(weights.astype(jnp.bfloat16), head_values, preferred_element_type=jnp.float32)
            return (mixed_rows / totals).astype(jnp.bfloat16)
        return lax.map(one_block, jnp.arange(PACKED_TOKENS // query_block, dtype=jnp.int32)).reshape(PACKED_TOKENS, HEAD_WIDTH)
    heads_out = lax.map(one_head, jnp.arange(QUERY_HEADS, dtype=jnp.int32))
    heads_out = heads_out.transpose(1, 0, 2).reshape(PACKED_TOKENS, QUERY_HEADS * HEAD_WIDTH)
    projected = jnp.dot(heads_out, output_weight, preferred_element_type=jnp.float32).astype(jnp.bfloat16)
    block_order = owner_order(block_owner, TOK_DEV // BLOCK)
    new_rows = (block_order[:, None] * BLOCK + jnp.arange(BLOCK, dtype=jnp.int32)[None, :]).reshape(-1)
    return jnp.take(projected, new_rows, axis=0)
```

```python
import functools
import math

import jax
import jax.numpy as jnp
from jax import lax
from jax.experimental import pallas as pl
from jax.experimental.pallas import tpu as pltpu
from jax.sharding import PartitionSpec as P

HEAD_WIDTH = 128
BLOCK = 128


rope_theta = 500000.0
rope_factor = 8.0
rope_context = 8192.0
masked_score = -1e30


def rope_inverse(head_size):
    halves = jnp.arange(head_size // 2, dtype=jnp.float32)
    inverse = 1.0 / rope_theta ** (2.0 * halves / head_size)
    wavelength = 2.0 * math.pi / inverse
    smooth = (rope_context / wavelength - 1.0) / 3.0
    blended = (1.0 - smooth) * inverse / rope_factor + smooth * inverse
    longer = jnp.where(wavelength > rope_context, inverse / rope_factor, blended)
    return jnp.where(wavelength < rope_context / 4.0, inverse, longer)


def document_of(tokens, bounds):
    inner_bounds = bounds[1:-1]
    return jnp.sum((tokens[:, None] >= inner_bounds[None, :]).astype(jnp.int32), axis=1)


def position_of(tokens, bounds):
    starts = bounds[:-1]
    document_start = jnp.max(
        jnp.where(starts[None, :] <= tokens[:, None], starts[None, :], 0), axis=1
    )
    return tokens - document_start


def rotate(raw_rows, tokens, bounds, head_size):
    row_count = raw_rows.shape[0]
    head_count = raw_rows.shape[1] // head_size
    angles = (
        position_of(tokens, bounds).astype(jnp.float32)[:, None] * rope_inverse(head_size)[None, :]
    )
    cosine = jnp.cos(angles)[:, None, :]
    sine_table = jnp.sin(angles)[:, None, :]
    heads_view = raw_rows.reshape(row_count, head_count, head_size)
    front_half = heads_view[:, :, : head_size // 2]
    back_half = heads_view[:, :, head_size // 2 :]
    turned = jnp.concatenate(
        [
            front_half * cosine - back_half * sine_table,
            back_half * cosine + front_half * sine_table,
        ],
        axis=2,
    )
    return turned.reshape(row_count, head_count * head_size).astype(jnp.bfloat16)


def owner_order(block_owner, per_device):
    block_count = block_owner.shape[0]
    blocks = jnp.arange(block_count, dtype=jnp.int32)
    same_owner = block_owner[:, None] == block_owner[None, :]
    earlier = blocks[None, :] < blocks[:, None]
    owner_rank = jnp.sum((same_owner & earlier).astype(jnp.int32), axis=1)
    target = block_owner * per_device + owner_rank
    return jnp.sum(jnp.where(target[None, :] == blocks[:, None], blocks[None, :], 0), axis=1)


def relayout(local_rows, block_order):
    cp_size = lax.axis_size("cp")
    row_count, row_width = local_rows.shape
    per_device = row_count // BLOCK
    portion = BLOCK // cp_size
    pieces = local_rows.reshape(per_device, cp_size, portion * row_width)
    spread = lax.all_to_all(pieces, "cp", split_axis=1, concat_axis=0, tiled=True)
    spread = spread.reshape(per_device * cp_size, portion * row_width)
    wanted = block_order.reshape(cp_size, per_device).T.reshape(-1)
    outgoing = jnp.take(spread, wanted, axis=0).reshape(per_device, cp_size, portion * row_width)
    arrived = lax.all_to_all(outgoing, "cp", split_axis=1, concat_axis=1, tiled=True)
    return arrived.reshape(row_count, row_width)


def project(local_rows, query_weight, key_matrix, value_matrix):
    weight_list = (query_weight, key_matrix, value_matrix)
    portion = lax.all_gather(local_rows, "tp", axis=1, tiled=True)
    return tuple(
        (jnp.dot(portion, weight, preferred_element_type=jnp.float32) for weight in weight_list)
    )


def attend(queries, query_tokens, key_rows, value_rows, key_tokens, bounds, head_size, kv_heads):
    row_count = queries.shape[0]
    query_group_width = queries.shape[1] // (kv_heads * head_size)
    grouped = queries.reshape(row_count, kv_heads, query_group_width, head_size).transpose(
        1, 2, 0, 3
    )
    grouped = grouped.reshape(kv_heads, query_group_width * row_count, head_size)
    query_documents = document_of(query_tokens, bounds)
    score_scale = 1.0 / math.sqrt(head_size)

    def update(flash_state, key_block, value_block, token_block):
        block_rows = key_block.shape[0]
        key_documents = document_of(token_block, bounds)
        allowed = (query_documents[:, None] == key_documents[None, :]) & (
            token_block[None, :] <= query_tokens[:, None]
        )
        running_max, running_sum, running_out = flash_state
        per_head_keys = key_block.reshape(block_rows, kv_heads, head_size).transpose(1, 0, 2)
        per_head_values = value_block.reshape(block_rows, kv_heads, head_size).transpose(1, 0, 2)
        scores = (
            jnp.einsum("khd,ksd->khs", grouped, per_head_keys, preferred_element_type=jnp.float32)
            * score_scale
        )
        wide_mask = jnp.tile(allowed, (query_group_width, 1))[None, :, :]
        scores = jnp.where(wide_mask, scores, masked_score)
        new_max = jnp.maximum(running_max, jnp.max(scores, axis=2))
        weights = jnp.where(wide_mask, jnp.exp(scores - new_max[:, :, None]), 0.0)
        factor = jnp.exp(running_max - new_max)
        new_sum = running_sum * factor + jnp.sum(weights, axis=2)
        new_out = running_out * factor[:, :, None] + jnp.einsum(
            "khs,ksd->khd",
            weights.astype(jnp.bfloat16),
            per_head_values,
            preferred_element_type=jnp.float32,
        )
        return (new_max, new_sum, new_out)

    initial = (
        jnp.full((kv_heads, query_group_width * row_count), masked_score, jnp.float32),
        jnp.zeros((kv_heads, query_group_width * row_count), jnp.float32),
        jnp.zeros((kv_heads, query_group_width * row_count, head_size), jnp.float32),
    )
    key_part = lax.all_gather(key_rows, "cp", axis=0, tiled=True)
    value_part = lax.all_gather(value_rows, "cp", axis=0, tiled=True)
    token_part = lax.all_gather(key_tokens, "cp", axis=0, tiled=True)
    part_rows = key_part.shape[0]
    block_rows = math.gcd(part_rows, 512)

    def one_block(block_index, inner_state):
        first_row = block_index * block_rows
        return update(
            inner_state,
            lax.dynamic_slice_in_dim(key_part, first_row, block_rows, 0),
            lax.dynamic_slice_in_dim(value_part, first_row, block_rows, 0),
            lax.dynamic_slice_in_dim(token_part, first_row, block_rows, 0),
        )

    final_max, final_sum, final_out = lax.fori_loop(0, part_rows // block_rows, one_block, initial)
    normalized = final_out / final_sum[:, :, None]
    merged = normalized.reshape(kv_heads, query_group_width, row_count, head_size).transpose(
        2, 0, 1, 3
    )
    return merged.reshape(row_count, kv_heads * query_group_width * head_size).astype(jnp.bfloat16)


def output_rows(heads_out, output_weight):
    head_terms = jnp.dot(heads_out, output_weight, preferred_element_type=jnp.float32)
    return lax.psum_scatter(head_terms.astype(jnp.bfloat16), "tp", scatter_dimension=1, tiled=True)


MESH = pl.DeviceIdType.MESH
WINDOW = 512


def dot(a, b):
    return jnp.dot(a, b, preferred_element_type=jnp.float32)


def turn(raw, cosine, sine):
    half = raw.shape[1] // 2
    swapped = jnp.concatenate([raw[:, half:], raw[:, :half]], axis=1)
    return (raw * cosine + swapped * sine).astype(jnp.bfloat16)


def greet(n_cp, n_tp):
    c, z = lax.axis_index("cp"), lax.axis_index("tp")
    barrier = pltpu.get_barrier_semaphore()
    for t in range(1, n_cp):
        peer = lax.rem(c + t, n_cp)
        pl.semaphore_signal(barrier, inc=1, device_id={"cp": peer}, device_id_type=MESH)
    for t in range(1, n_tp):
        peer = lax.rem(z + t, n_tp)
        pl.semaphore_signal(barrier, inc=1, device_id={"tp": peer}, device_id_type=MESH)
    pl.semaphore_wait(barrier, n_cp + n_tp - 2)


def project_kernel(
    n_cp, n_tp,
    hidden, wq_hbm, wk_hbm, wv_hbm, cosine, sine,
    q_out, kv_out,
    rows, wq, wkv, acc_q, acc_kv, kv_own, kv_all,
    w_sem, own_sem, s_send, s_recv, r_send, l_send, z_recv, k_send, k_recv, d_send, d_recv, kown_sem,
):
    c, z = lax.axis_index("cp"), lax.axis_index("tp")
    per = hidden.shape[0]
    width = hidden.shape[3]
    weights = (
        pltpu.make_async_copy(wq_hbm, wq, w_sem.at[0]),
        pltpu.make_async_copy(wk_hbm, wkv.at[:, pl.ds(0, HEAD_WIDTH)], w_sem.at[1]),
        pltpu.make_async_copy(wv_hbm, wkv.at[:, pl.ds(HEAD_WIDTH, HEAD_WIDTH)], w_sem.at[2]),
    )
    own = pltpu.make_async_copy(hidden.at[:, c], rows.at[z, pl.ds(c * per, per)], own_sem)
    own.start()
    greet(n_cp, n_tp)

    def spread(t):
        peer = lax.rem(c + t, n_cp)
        return pltpu.make_async_remote_copy(
            src_ref=hidden.at[:, peer], dst_ref=rows.at[z, pl.ds(c * per, per)],
            send_sem=s_send.at[t], recv_sem=s_recv.at[t],
            device_id={"cp": peer}, device_id_type=MESH,
        )

    def along(origin, t, step):
        source = lax.rem(c - t + n_cp, n_cp)
        piece = rows.at[origin, pl.ds(source * per, per)]
        sems = r_send if step > 0 else l_send
        return pltpu.make_async_remote_copy(
            src_ref=piece, dst_ref=piece,
            send_sem=sems.at[origin, t], recv_sem=z_recv.at[origin, t],
            device_id={"tp": lax.rem(z + step + n_tp, n_tp)}, device_id_type=MESH,
        )

    def multiply(origin, first):
        block = rows[origin].reshape(-1, width)
        span = pl.ds(pl.multiple_of(origin * width, width), width)
        kv_term = dot(block, wkv[span, :])
        q_term = dot(block, wq[span, :])
        if first:
            acc_kv[...] = kv_term
            acc_q[...] = q_term
        else:
            acc_kv[...] += kv_term
            acc_q[...] += q_term

    for t in range(1, n_cp):
        spread(t).start()
    for copy in weights:
        copy.start()
    for t in range(n_cp):
        if t == 0:
            own.wait()
        else:
            spread(t).wait_recv()

        @pl.when(z < n_tp - 1)
        def _():
            along(z, t, 1).start()

        @pl.when(z > 0)
        def _():
            along(z, t, -1).start()

    for copy in weights:
        copy.wait()
    multiply(z, True)

    @pl.loop(1, n_tp)
    def _(s):
        for t in range(n_cp):
            @pl.when(z - s >= 0)
            def _():
                along(z - s, t, 1).wait_recv()

                @pl.when(z < n_tp - 1)
                def _():
                    along(z - s, t, 1).start()

            @pl.when(z + s < n_tp)
            def _():
                along(z + s, t, -1).wait_recv()

                @pl.when(z > 0)
                def _():
                    along(z + s, t, -1).start()

        @pl.when(z - s >= 0)
        def _():
            multiply(z - s, False)

        @pl.when(z + s < n_tp)
        def _():
            multiply(z + s, False)

    key = turn(acc_kv[:, :HEAD_WIDTH], cosine[...], sine[...])
    value = acc_kv[:, HEAD_WIDTH:].astype(jnp.bfloat16)
    kv_own[...] = jnp.concatenate([key, value], axis=1).reshape(kv_own.shape)
    chips = n_cp // 2
    partner = c + 1 - 2 * lax.rem(c, 2)
    mine = pltpu.make_async_copy(kv_own, kv_all.at[:, c], kown_sem)

    def across(i):
        return pltpu.make_async_remote_copy(
            src_ref=kv_own, dst_ref=kv_all.at[:, c],
            send_sem=k_send.at[i], recv_sem=k_recv.at[i],
            device_id={"cp": lax.rem(c + 2 * i, n_cp)}, device_id_type=MESH,
        )

    def handed(i):
        source = lax.rem(c - 2 * i + n_cp, n_cp)
        return pltpu.make_async_remote_copy(
            src_ref=kv_own if i == 0 else kv_all.at[:, source], dst_ref=kv_all.at[:, source],
            send_sem=d_send.at[i], recv_sem=d_recv.at[i],
            device_id={"cp": partner}, device_id_type=MESH,
        )

    for i in range(1, chips):
        across(i).start()
    handed(0).start()
    mine.start()
    for h in range(q_out.shape[1] // HEAD_WIDTH):
        cols = slice(h * HEAD_WIDTH, (h + 1) * HEAD_WIDTH)
        q_out[:, cols] = turn(acc_q[:, cols], cosine[...], sine[...])
    for i in range(1, chips):
        across(i).wait_recv()
        handed(i).start()
    mine.wait()
    for i in range(chips):
        handed(i).wait_recv()
    kv_out[...] = kv_all[...]
    for t in range(1, n_cp):
        spread(t).wait_send()
    for t in range(n_cp):
        for o in range(n_tp):
            @pl.when((z < n_tp - 1) & (o <= z))
            def _():
                along(o, t, 1).wait_send()

            @pl.when((z > 0) & (o >= z))
            def _():
                along(o, t, -1).wait_send()
    for i in range(1, chips):
        across(i).wait_send()
    for i in range(chips):
        handed(i).wait_send()


def project_call(hidden, wq, wk, wv, cosine, sine, n_cp, n_tp):
    rows, width = hidden.shape
    per = rows // BLOCK
    share = BLOCK // n_cp
    blocks = per * n_cp
    pieces = hidden.reshape(per, n_cp, share, width)
    bf, dma = jnp.bfloat16, pltpu.SemaphoreType.DMA
    vmem = pl.BlockSpec(memory_space=pltpu.VMEM)
    hbm = pl.BlockSpec(memory_space=pl.ANY)
    flops = 2 * rows * wq.shape[0] * (wq.shape[1] + 2 * HEAD_WIDTH)
    return pl.pallas_call(
        functools.partial(project_kernel, n_cp, n_tp),
        out_shape=(
            jax.ShapeDtypeStruct((rows, wq.shape[1]), bf),
            jax.ShapeDtypeStruct((blocks, n_cp, share, 2 * HEAD_WIDTH), bf),
        ),
        in_specs=[vmem, hbm, hbm, hbm, vmem, vmem],
        out_specs=(vmem, vmem),
        scratch_shapes=[
            pltpu.VMEM((n_tp, blocks, share, width), bf),
            pltpu.VMEM(wq.shape, bf),
            pltpu.VMEM((wq.shape[0], 2 * HEAD_WIDTH), bf),
            pltpu.VMEM((rows, wq.shape[1]), jnp.float32),
            pltpu.VMEM((rows, 2 * HEAD_WIDTH), jnp.float32),
            pltpu.VMEM((blocks, share, 2 * HEAD_WIDTH), bf),
            pltpu.VMEM((blocks, n_cp, share, 2 * HEAD_WIDTH), bf),
            dma((3,)), dma, dma((n_cp,)), dma((n_cp,)),
            dma((n_tp, n_cp)), dma((n_tp, n_cp)), dma((n_tp, n_cp)),
            dma((n_cp,)), dma((n_cp,)), dma((n_cp,)), dma((n_cp,)), dma,
        ],
        compiler_params=pltpu.CompilerParams(
            collective_id=1, has_side_effects=True, vmem_limit_bytes=48 << 20
        ),
        cost_estimate=pl.CostEstimate(flops=flops, bytes_accessed=12 << 20, transcendentals=0),
    )(pieces, wq, wk, wv, cosine, sine)


def attend_kernel(first_key, where, q_ref, kv_ref, start_ref, token_ref, out_ref, *, heads):
    blocks, share = q_ref.shape[0], q_ref.shape[1]
    scale = 1.0 / math.sqrt(HEAD_WIDTH)
    keys = kv_ref.shape[0]
    window = min(WINDOW, keys)

    def stack(tile):
        return jnp.concatenate(
            [tile[:, h * HEAD_WIDTH : (h + 1) * HEAD_WIDTH] for h in range(heads)], axis=0
        )

    def scored(q, begin, stop, start, token):
        span = pl.ds(pl.multiple_of(begin, BLOCK), window)
        key = kv_ref[span, :HEAD_WIDTH]
        value = kv_ref[span, HEAD_WIDTH:]
        score = lax.dot_general(
            q, key, (((1,), (1,)), ((), ())), preferred_element_type=jnp.float32
        ) * scale
        index = begin + lax.broadcasted_iota(jnp.int32, score.shape, 1)
        allowed = (index >= start) & (index <= token) & (index < stop)
        return jnp.where(allowed, score, masked_score), allowed, value

    def one(b):
        q = stack(q_ref[b])
        start = jnp.tile(start_ref[b], (heads, 1))[:, :1]
        token = jnp.tile(token_ref[b], (heads, 1))[:, :1]
        stop = (b + 1) * BLOCK
        begin = jnp.maximum(stop - window, 0)
        score, allowed, value = scored(q, begin, stop, start, token)
        top = jnp.max(score, axis=1, keepdims=True)
        weight = jnp.where(allowed, jnp.exp(score - top), 0.0)
        total = jnp.sum(weight, axis=1, keepdims=True)
        out = dot(weight.astype(jnp.bfloat16), value)
        low = first_key[b]

        def more(carry):
            stop, top, total, out = carry
            begin = jnp.maximum(stop - window, 0)
            score, allowed, value = scored(q, begin, stop, start, token)
            new_top = jnp.maximum(top, jnp.max(score, axis=1, keepdims=True))
            weight = jnp.where(allowed, jnp.exp(score - new_top), 0.0)
            factor = jnp.exp(top - new_top)
            total = total * factor + jnp.sum(weight, axis=1, keepdims=True)
            out = out * factor + dot(weight.astype(jnp.bfloat16), value)
            return begin, new_top, total, out

        return low, more, (begin, top, total, out)

    group = 4

    @pl.loop(0, blocks // group)
    def _(g):
        firsts = [one(g * group + i) for i in range(group)]
        for i, (low, more, carry) in enumerate(firsts):
            _, _, total, out = lax.while_loop(lambda state: state[0] > low, more, carry)
            out = (out / total).astype(jnp.bfloat16)
            tile = jnp.concatenate(
                [out[h * share : (h + 1) * share] for h in range(heads)], axis=1
            )
            out_ref[where[g * group + i]] = tile


def attend_call(q, kv, first_key, where, start, token, n_cp):
    rows, width = q.shape
    share = BLOCK // n_cp
    blocks = rows // share
    vmem = pl.BlockSpec(memory_space=pltpu.VMEM)
    smem = pl.BlockSpec(memory_space=pltpu.SMEM)
    lanes = lambda a: jnp.broadcast_to(a.reshape(blocks, share, 1), (blocks, share, HEAD_WIDTH))
    return pl.pallas_call(
        functools.partial(attend_kernel, heads=width // HEAD_WIDTH),
        out_shape=jax.ShapeDtypeStruct((blocks, share, width), jnp.bfloat16),
        in_specs=[smem, smem, vmem, vmem, vmem, vmem],
        out_specs=vmem,
        compiler_params=pltpu.CompilerParams(vmem_limit_bytes=32 << 20),
    )(
        first_key, where, q.reshape(blocks, share, width),
        kv.reshape(-1, 2 * HEAD_WIDTH), lanes(start), lanes(token),
    )


def output_kernel(
    n_cp, n_tp, heads, wo_hbm, out_ref,
    wo, part, from_left, from_right, to_right, to_left, done, landed,
    w_sem, r_send, l_send, r_recv, l_recv, a_send, a_recv,
):
    c, z = lax.axis_index("cp"), lax.axis_index("tp")
    per = out_ref.shape[0]
    share, width = heads.shape[1], out_ref.shape[3]

    def weight(o):
        cols = pl.ds(pl.multiple_of(o * width, width), width)
        return pltpu.make_async_copy(wo_hbm.at[:, cols], wo.at[o], w_sem.at[o])

    for s in range(n_tp - 1, -1, -1):
        @pl.when(z + s < n_tp)
        def _():
            weight(z + s).start()

        if s > 0:
            @pl.when(z - s >= 0)
            def _():
                weight(z - s).start()

    greet(n_cp, n_tp)

    def piece(t):
        return pl.ds(lax.rem(c + t, n_cp) * per, per)

    def rightward(o, t):
        return pltpu.make_async_remote_copy(
            src_ref=to_right.at[o, piece(t)], dst_ref=from_left.at[o, piece(t)],
            send_sem=r_send.at[o, t], recv_sem=r_recv.at[o, t],
            device_id={"tp": lax.rem(z + 1, n_tp)}, device_id_type=MESH,
        )

    def leftward(o, t):
        return pltpu.make_async_remote_copy(
            src_ref=to_left.at[o, piece(t)], dst_ref=from_right.at[o, piece(t)],
            send_sem=l_send.at[o, t], recv_sem=l_recv.at[o, t],
            device_id={"tp": lax.rem(z + n_tp - 1, n_tp)}, device_id_type=MESH,
        )

    def final(t):
        peer = lax.rem(c + t, n_cp)
        return pltpu.make_async_remote_copy(
            src_ref=done.at[piece(t)], dst_ref=landed.at[:, c],
            send_sem=a_send.at[t], recv_sem=a_recv.at[t],
            device_id={"cp": peer}, device_id_type=MESH,
        )

    def term(o):
        weight(o).wait()
        block = heads[...].reshape(-1, heads.shape[2])
        return dot(block, wo[o]).reshape(part.shape[1:])

    order = list(range(1, n_cp)) + [0]

    @pl.loop(0, n_tp - 1)
    def _(i):
        s = n_tp - 1 - i

        @pl.when(z + s < n_tp)
        def _():
            product = term(z + s)

            @pl.when(z == 0)
            def _():
                to_right[z + s] = product.astype(jnp.bfloat16)
                for t in order:
                    rightward(z + s, t).start()

            @pl.when(z > 0)
            def _():
                part[z + s] = product

        @pl.when(z - s >= 0)
        def _():
            product = term(z - s)

            @pl.when(z == n_tp - 1)
            def _():
                to_left[z - s] = product.astype(jnp.bfloat16)
                for t in order:
                    leftward(z - s, t).start()

            @pl.when(z < n_tp - 1)
            def _():
                part[z - s] = product

    part[z] = term(z)

    @pl.loop(0, n_tp - 1)
    def _(i):
        s = n_tp - 1 - i
        for t in order:
            @pl.when((z + s < n_tp) & (z > 0))
            def _():
                rightward(z + s, t).wait_recv()
                total = part[z + s, piece(t)] + from_left[z + s, piece(t)].astype(jnp.float32)
                to_right[z + s, piece(t)] = total.astype(jnp.bfloat16)
                rightward(z + s, t).start()

            @pl.when((z - s >= 0) & (z < n_tp - 1))
            def _():
                leftward(z - s, t).wait_recv()
                total = part[z - s, piece(t)] + from_right[z - s, piece(t)].astype(jnp.float32)
                to_left[z - s, piece(t)] = total.astype(jnp.bfloat16)
                leftward(z - s, t).start()

    for t in order:
        @pl.when(z > 0)
        def _():
            rightward(z, t).wait_recv()
            part[z, piece(t)] += from_left[z, piece(t)].astype(jnp.float32)

        @pl.when(z < n_tp - 1)
        def _():
            leftward(z, t).wait_recv()
            part[z, piece(t)] += from_right[z, piece(t)].astype(jnp.float32)

        done[piece(t)] = part[z, piece(t)].astype(jnp.bfloat16)
        if t > 0:
            final(t).start()

    for t in range(1, n_cp):
        final(t).wait_recv()
        source = lax.rem(c - t + n_cp, n_cp)
        out_ref[:, pl.ds(source, 1)] = landed[:, pl.ds(source, 1)]
    out_ref[:, pl.ds(c, 1)] = done[piece(0)][:, None]
    for t in range(1, n_cp):
        final(t).wait_send()
    for t in range(n_cp):
        for o in range(n_tp):
            @pl.when(o > z)
            def _():
                rightward(o, t).wait_send()

            @pl.when(o < z)
            def _():
                leftward(o, t).wait_send()


def output_call(heads, wo, n_cp, n_tp):
    blocks, share, depth = heads.shape
    width = wo.shape[1] // n_tp
    per = blocks // n_cp
    bf, dma = jnp.bfloat16, pltpu.SemaphoreType.DMA
    vmem = pl.BlockSpec(memory_space=pltpu.VMEM)
    slab = (n_tp, blocks, share, width)
    out = pl.pallas_call(
        functools.partial(output_kernel, n_cp, n_tp),
        out_shape=jax.ShapeDtypeStruct((per, n_cp, share, width), bf),
        in_specs=[vmem, pl.BlockSpec(memory_space=pl.ANY)],
        out_specs=vmem,
        scratch_shapes=[
            pltpu.VMEM((n_tp, depth, width), bf),
            pltpu.VMEM(slab, jnp.float32),
            pltpu.VMEM(slab, bf), pltpu.VMEM(slab, bf), pltpu.VMEM(slab, bf), pltpu.VMEM(slab, bf),
            pltpu.VMEM(slab[1:], bf),
            pltpu.VMEM((per, n_cp, share, width), bf),
            dma((n_tp,)), dma((n_tp, n_cp)), dma((n_tp, n_cp)), dma((n_tp, n_cp)), dma((n_tp, n_cp)),
            dma((n_cp,)), dma((n_cp,)),
        ],
        compiler_params=pltpu.CompilerParams(
            collective_id=2, has_side_effects=True, vmem_limit_bytes=48 << 20
        ),
        cost_estimate=pl.CostEstimate(
            flops=2 * blocks * share * depth * wo.shape[1], bytes_accessed=12 << 20, transcendentals=0
        ),
    )(heads, wo)
    return out.reshape(per * n_cp * share, width)


def local_fused(
    hidden, query_weight, key_matrix, value_matrix, output_weight, document_bounds, block_owner
):
    n_cp, n_tp = lax.axis_size("cp"), lax.axis_size("tp")
    c = lax.axis_index("cp")
    per = hidden.shape[0] // BLOCK
    share = BLOCK // n_cp
    blocks = block_owner.shape[0]
    index = jnp.arange(blocks, dtype=jnp.int32)
    tokens = (
        index[:, None] * BLOCK + c * share + jnp.arange(share, dtype=jnp.int32)[None, :]
    ).reshape(-1)
    position = position_of(tokens, document_bounds)
    angles = position.astype(jnp.float32)[:, None] * rope_inverse(HEAD_WIDTH)[None, :]
    cosine, sine = jnp.cos(angles), jnp.sin(angles)
    cosine = jnp.concatenate([cosine, cosine], axis=1)
    sine = jnp.concatenate([-sine, sine], axis=1)
    starts = tokens - position
    first_key = jnp.min(starts.reshape(blocks, share), axis=1)
    same_owner = block_owner[:, None] == block_owner[None, :]
    rank = jnp.sum((same_owner & (index[None, :] < index[:, None])).astype(jnp.int32), axis=1)
    slot = block_owner * per + rank
    q, kv = project_call(
        hidden, query_weight, key_matrix, value_matrix, cosine, sine, n_cp, n_tp
    )
    heads = attend_call(q, kv, first_key, slot, starts, tokens, n_cp)
    return output_call(heads, output_weight, n_cp, n_tp)


def local_plain(
    hidden, query_weight, key_matrix, value_matrix, output_weight, document_bounds, block_owner
):
    cp_index = lax.axis_index("cp")
    row_count = hidden.shape[0]
    per_device = row_count // BLOCK
    block_order = owner_order(block_owner, per_device)
    own_blocks = lax.dynamic_slice_in_dim(block_order, cp_index * per_device, per_device, 0)
    new_tokens = (
        own_blocks[:, None] * BLOCK + jnp.arange(BLOCK, dtype=jnp.int32)[None, :]
    ).reshape(-1)
    kv_heads = key_matrix.shape[1] // HEAD_WIDTH
    moved = relayout(hidden, block_order)
    query_raw, key_raw, value_raw = project(moved, query_weight, key_matrix, value_matrix)
    queries = rotate(query_raw, new_tokens, document_bounds, HEAD_WIDTH)
    key_rows = rotate(key_raw, new_tokens, document_bounds, HEAD_WIDTH)
    value_rows = value_raw.astype(jnp.bfloat16)
    heads_out = attend(
        queries, new_tokens, key_rows, value_rows, new_tokens, document_bounds, HEAD_WIDTH, kv_heads
    )
    return output_rows(heads_out, output_weight)


def solution(mesh):
    shares = BLOCK // mesh.shape["cp"]
    local = local_fused if shares % 16 == 0 else local_plain
    placed = (P("cp", "tp"), P(None, "tp"), P(None, "tp"), P(None, "tp"), P("tp", None), P(), P())
    return jax.shard_map(
        local, mesh=mesh, in_specs=placed, out_specs=P("cp", "tp"), check_vma=False
    )
```

```python
import functools
import math

import jax
import jax.numpy as jnp
from jax import lax
from jax.experimental import pallas as pl
from jax.experimental.pallas import tpu as pltpu
from jax.sharding import PartitionSpec as P

HEAD_WIDTH = 128
BLOCK = 128


rope_theta = 500000.0
rope_factor = 8.0
rope_context = 8192.0
masked_score = -1e30


def rope_inverse(head_size):
    halves = jnp.arange(head_size // 2, dtype=jnp.float32)
    inverse = 1.0 / rope_theta ** (2.0 * halves / head_size)
    wavelength = 2.0 * math.pi / inverse
    smooth = (rope_context / wavelength - 1.0) / 3.0
    blended = (1.0 - smooth) * inverse / rope_factor + smooth * inverse
    longer = jnp.where(wavelength > rope_context, inverse / rope_factor, blended)
    return jnp.where(wavelength < rope_context / 4.0, inverse, longer)


def document_of(tokens, bounds):
    inner_bounds = bounds[1:-1]
    return jnp.sum((tokens[:, None] >= inner_bounds[None, :]).astype(jnp.int32), axis=1)


def position_of(tokens, bounds):
    starts = bounds[:-1]
    document_start = jnp.max(
        jnp.where(starts[None, :] <= tokens[:, None], starts[None, :], 0), axis=1
    )
    return tokens - document_start


def rotate(raw_rows, tokens, bounds, head_size):
    row_count = raw_rows.shape[0]
    head_count = raw_rows.shape[1] // head_size
    angles = (
        position_of(tokens, bounds).astype(jnp.float32)[:, None] * rope_inverse(head_size)[None, :]
    )
    cosine = jnp.cos(angles)[:, None, :]
    sine_table = jnp.sin(angles)[:, None, :]
    heads_view = raw_rows.reshape(row_count, head_count, head_size)
    front_half = heads_view[:, :, : head_size // 2]
    back_half = heads_view[:, :, head_size // 2 :]
    turned = jnp.concatenate(
        [
            front_half * cosine - back_half * sine_table,
            back_half * cosine + front_half * sine_table,
        ],
        axis=2,
    )
    return turned.reshape(row_count, head_count * head_size).astype(jnp.bfloat16)


def owner_order(block_owner, per_device):
    block_count = block_owner.shape[0]
    blocks = jnp.arange(block_count, dtype=jnp.int32)
    same_owner = block_owner[:, None] == block_owner[None, :]
    earlier = blocks[None, :] < blocks[:, None]
    owner_rank = jnp.sum((same_owner & earlier).astype(jnp.int32), axis=1)
    target = block_owner * per_device + owner_rank
    return jnp.sum(jnp.where(target[None, :] == blocks[:, None], blocks[None, :], 0), axis=1)


def relayout(local_rows, block_order):
    cp_size = lax.axis_size("cp")
    row_count, row_width = local_rows.shape
    per_device = row_count // BLOCK
    portion = BLOCK // cp_size
    pieces = local_rows.reshape(per_device, cp_size, portion * row_width)
    spread = lax.all_to_all(pieces, "cp", split_axis=1, concat_axis=0, tiled=True)
    spread = spread.reshape(per_device * cp_size, portion * row_width)
    wanted = block_order.reshape(cp_size, per_device).T.reshape(-1)
    outgoing = jnp.take(spread, wanted, axis=0).reshape(per_device, cp_size, portion * row_width)
    arrived = lax.all_to_all(outgoing, "cp", split_axis=1, concat_axis=1, tiled=True)
    return arrived.reshape(row_count, row_width)


def project(local_rows, query_weight, key_matrix, value_matrix):
    weight_list = (query_weight, key_matrix, value_matrix)
    portion = lax.all_gather(local_rows, "tp", axis=1, tiled=True)
    return tuple(
        (jnp.dot(portion, weight, preferred_element_type=jnp.float32) for weight in weight_list)
    )


def attend(queries, query_tokens, key_rows, value_rows, key_tokens, bounds, head_size, kv_heads):
    row_count = queries.shape[0]
    query_group_width = queries.shape[1] // (kv_heads * head_size)
    grouped = queries.reshape(row_count, kv_heads, query_group_width, head_size).transpose(
        1, 2, 0, 3
    )
    grouped = grouped.reshape(kv_heads, query_group_width * row_count, head_size)
    query_documents = document_of(query_tokens, bounds)
    score_scale = 1.0 / math.sqrt(head_size)

    def update(flash_state, key_block, value_block, token_block):
        block_rows = key_block.shape[0]
        key_documents = document_of(token_block, bounds)
        allowed = (query_documents[:, None] == key_documents[None, :]) & (
            token_block[None, :] <= query_tokens[:, None]
        )
        running_max, running_sum, running_out = flash_state
        per_head_keys = key_block.reshape(block_rows, kv_heads, head_size).transpose(1, 0, 2)
        per_head_values = value_block.reshape(block_rows, kv_heads, head_size).transpose(1, 0, 2)
        scores = (
            jnp.einsum("khd,ksd->khs", grouped, per_head_keys, preferred_element_type=jnp.float32)
            * score_scale
        )
        wide_mask = jnp.tile(allowed, (query_group_width, 1))[None, :, :]
        scores = jnp.where(wide_mask, scores, masked_score)
        new_max = jnp.maximum(running_max, jnp.max(scores, axis=2))
        weights = jnp.where(wide_mask, jnp.exp(scores - new_max[:, :, None]), 0.0)
        factor = jnp.exp(running_max - new_max)
        new_sum = running_sum * factor + jnp.sum(weights, axis=2)
        new_out = running_out * factor[:, :, None] + jnp.einsum(
            "khs,ksd->khd",
            weights.astype(jnp.bfloat16),
            per_head_values,
            preferred_element_type=jnp.float32,
        )
        return (new_max, new_sum, new_out)

    initial = (
        jnp.full((kv_heads, query_group_width * row_count), masked_score, jnp.float32),
        jnp.zeros((kv_heads, query_group_width * row_count), jnp.float32),
        jnp.zeros((kv_heads, query_group_width * row_count, head_size), jnp.float32),
    )
    key_part = lax.all_gather(key_rows, "cp", axis=0, tiled=True)
    value_part = lax.all_gather(value_rows, "cp", axis=0, tiled=True)
    token_part = lax.all_gather(key_tokens, "cp", axis=0, tiled=True)
    part_rows = key_part.shape[0]
    block_rows = math.gcd(part_rows, 512)

    def one_block(block_index, inner_state):
        first_row = block_index * block_rows
        return update(
            inner_state,
            lax.dynamic_slice_in_dim(key_part, first_row, block_rows, 0),
            lax.dynamic_slice_in_dim(value_part, first_row, block_rows, 0),
            lax.dynamic_slice_in_dim(token_part, first_row, block_rows, 0),
        )

    final_max, final_sum, final_out = lax.fori_loop(0, part_rows // block_rows, one_block, initial)
    normalized = final_out / final_sum[:, :, None]
    merged = normalized.reshape(kv_heads, query_group_width, row_count, head_size).transpose(
        2, 0, 1, 3
    )
    return merged.reshape(row_count, kv_heads * query_group_width * head_size).astype(jnp.bfloat16)


def output_rows(heads_out, output_weight):
    head_terms = jnp.dot(heads_out, output_weight, preferred_element_type=jnp.float32)
    return lax.psum_scatter(head_terms.astype(jnp.bfloat16), "tp", scatter_dimension=1, tiled=True)


MESH = pl.DeviceIdType.MESH
WINDOW = 512


def dot(a, b):
    return jnp.dot(a, b, preferred_element_type=jnp.float32)


def turn(raw, cosine, sine):
    half = raw.shape[1] // 2
    swapped = jnp.concatenate([raw[:, half:], raw[:, :half]], axis=1)
    return (raw * cosine + swapped * sine).astype(jnp.bfloat16)


def greet(n_cp, n_tp):
    c, z = lax.axis_index("cp"), lax.axis_index("tp")
    barrier = pltpu.get_barrier_semaphore()
    for t in range(1, n_cp):
        peer = lax.rem(c + t, n_cp)
        pl.semaphore_signal(barrier, inc=1, device_id={"cp": peer}, device_id_type=MESH)
    for t in range(1, n_tp):
        peer = lax.rem(z + t, n_tp)
        pl.semaphore_signal(barrier, inc=1, device_id={"tp": peer}, device_id_type=MESH)
    pl.semaphore_wait(barrier, n_cp + n_tp - 2)


def row_tokens(bounds, blocks, share, offset):
    shape = (blocks, share, HEAD_WIDTH)
    token = (
        lax.broadcasted_iota(jnp.int32, shape, 0) * BLOCK
        + lax.broadcasted_iota(jnp.int32, shape, 1) + offset
    )
    start = jnp.zeros_like(token)
    for i in range(bounds.shape[0] - 1):
        start = jnp.where(token >= bounds[i], bounds[i], start)
    return token, start


def project_kernel(
    n_cp, n_tp,
    bounds, hidden, wq_hbm, wk_hbm, wv_hbm, inverse,
    q_out, kv_out,
    rows, wq, wkv, acc_q, acc_kv, kv_own, kv_all, cosine, sine,
    w_sem, own_sem, s_send, s_recv, r_send, l_send, z_recv, k_send, k_recv, d_send, d_recv,
):
    c, z = lax.axis_index("cp"), lax.axis_index("tp")
    per = hidden.shape[0]
    width = hidden.shape[3]
    weights = (
        pltpu.make_async_copy(wq_hbm, wq, w_sem.at[0]),
        pltpu.make_async_copy(wk_hbm, wkv.at[:, pl.ds(0, HEAD_WIDTH)], w_sem.at[1]),
        pltpu.make_async_copy(wv_hbm, wkv.at[:, pl.ds(HEAD_WIDTH, HEAD_WIDTH)], w_sem.at[2]),
    )
    own = pltpu.make_async_copy(hidden.at[:, c], rows.at[z, pl.ds(c * per, per)], own_sem)
    own.start()
    greet(n_cp, n_tp)

    def spread(t):
        peer = lax.rem(c + t, n_cp)
        return pltpu.make_async_remote_copy(
            src_ref=hidden.at[:, peer], dst_ref=rows.at[z, pl.ds(c * per, per)],
            send_sem=s_send.at[t], recv_sem=s_recv.at[t],
            device_id={"cp": peer}, device_id_type=MESH,
        )

    def along(origin, t, step):
        source = lax.rem(c - t + n_cp, n_cp)
        piece = rows.at[origin, pl.ds(source * per, per)]
        sems = r_send if step > 0 else l_send
        return pltpu.make_async_remote_copy(
            src_ref=piece, dst_ref=piece,
            send_sem=sems.at[origin, t], recv_sem=z_recv.at[origin, t],
            device_id={"tp": lax.rem(z + step + n_tp, n_tp)}, device_id_type=MESH,
        )

    def multiply(origin, first):
        block = rows[origin].reshape(-1, width)
        span = pl.ds(pl.multiple_of(origin * width, width), width)
        kv_term = dot(block, wkv[span, :])
        q_term = dot(block, wq[span, :])
        if first:
            acc_kv[...] = kv_term
            acc_q[...] = q_term
        else:
            acc_kv[...] += kv_term
            acc_q[...] += q_term

    for t in range(1, n_cp):
        spread(t).start()
    for copy in weights:
        copy.start()
    for t in range(n_cp):
        if t == 0:
            own.wait()
        else:
            spread(t).wait_recv()

        @pl.when(z < n_tp - 1)
        def _():
            along(z, t, 1).start()

        @pl.when(z > 0)
        def _():
            along(z, t, -1).start()

    blocks, share = kv_own.shape[0], kv_own.shape[1]
    token, start = row_tokens(bounds, blocks, share, c * share)
    angle = (token - start).astype(jnp.float32).reshape(-1, HEAD_WIDTH) * inverse[...]
    cosine[...] = jnp.cos(angle)
    lane = lax.broadcasted_iota(jnp.int32, angle.shape, 1)
    sine[...] = jnp.where(lane < HEAD_WIDTH // 2, -1.0, 1.0) * jnp.sin(angle)
    for copy in weights:
        copy.wait()
    multiply(z, True)

    @pl.loop(1, n_tp - 1)
    def _(s):
        for t in range(n_cp):
            @pl.when(z - s >= 0)
            def _():
                along(z - s, t, 1).wait_recv()

                @pl.when(z < n_tp - 1)
                def _():
                    along(z - s, t, 1).start()

            @pl.when(z + s < n_tp)
            def _():
                along(z + s, t, -1).wait_recv()

                @pl.when(z > 0)
                def _():
                    along(z + s, t, -1).start()

        @pl.when(z - s >= 0)
        def _():
            multiply(z - s, False)

        @pl.when(z + s < n_tp)
        def _():
            multiply(z + s, False)

    chips = n_cp // 2
    partner = c + 1 - 2 * lax.rem(c, 2)
    count = per * share
    far = n_tp - 1 - z
    last = (z == 0) | (z == n_tp - 1)
    far_span = pl.ds(pl.multiple_of(far * width, width), width)

    def part_of(t):
        return lax.rem(c - t + n_cp, n_cp)

    def across(i, t):
        span = pl.ds(part_of(t) * per, per)
        return pltpu.make_async_remote_copy(
            src_ref=kv_own.at[span], dst_ref=kv_all.at[span, c],
            send_sem=k_send.at[i, t], recv_sem=k_recv.at[i, t],
            device_id={"cp": lax.rem(c + 2 * i, n_cp)}, device_id_type=MESH,
        )

    def arrived(i, t):
        source = lax.rem(c - 2 * i + n_cp, n_cp)
        span = pl.ds(lax.rem(source - t + n_cp, n_cp) * per, per)
        landed = kv_all.at[span, source]
        return pltpu.make_async_remote_copy(
            src_ref=landed, dst_ref=landed,
            send_sem=d_send.at[i, t], recv_sem=d_recv.at[i, t],
            device_id={"cp": partner}, device_id_type=MESH,
        )

    def handed(t):
        span = pl.ds(part_of(t) * per, per)
        return pltpu.make_async_remote_copy(
            src_ref=kv_own.at[span], dst_ref=kv_all.at[span, c],
            send_sem=d_send.at[0, t], recv_sem=d_recv.at[0, t],
            device_id={"cp": partner}, device_id_type=MESH,
        )

    @pl.loop(0, n_cp)
    def _(t):
        span = pl.ds(part_of(t) * per, per)
        lines = pl.ds(pl.multiple_of(part_of(t) * count, count), count)

        @pl.when(last)
        def _():
            along(far, t, 1).wait_recv()
            block = rows[far, span].reshape(count, width)
            acc_kv[lines, :] += dot(block, wkv[far_span, :])

        cos_t, sin_t = cosine[lines, :], sine[lines, :]
        key = turn(acc_kv[lines, :HEAD_WIDTH], cos_t, sin_t)
        value = acc_kv[lines, HEAD_WIDTH:].astype(jnp.bfloat16)
        tile = jnp.concatenate([key, value], axis=1).reshape(per, share, 2 * HEAD_WIDTH)
        kv_own[span] = tile
        kv_all[span, pl.ds(c, 1)] = tile[:, None]
        for i in range(1, chips):
            across(i, t).start()
        handed(t).start()

        @pl.when(last)
        def _():
            block = rows[far, span].reshape(count, width)
            acc_q[lines, :] += dot(block, wq[far_span, :])

        for h in range(q_out.shape[1] // HEAD_WIDTH):
            cols = slice(h * HEAD_WIDTH, (h + 1) * HEAD_WIDTH)
            q_out[lines, cols] = turn(acc_q[lines, cols], cos_t, sin_t)

    @pl.loop(0, n_cp)
    def _(t):
        for i in range(1, chips):
            across(i, t).wait_recv()
            arrived(i, t).start()

    @pl.loop(0, n_cp)
    def _(t):
        handed(t).wait_recv()
        for i in range(1, chips):
            arrived(i, t).wait_recv()

    kv_out[...] = kv_all[...]
    for t in range(1, n_cp):
        spread(t).wait_send()
    for t in range(n_cp):
        for o in range(n_tp):
            @pl.when((z < n_tp - 1) & (o <= z))
            def _():
                along(o, t, 1).wait_send()

            @pl.when((z > 0) & (o >= z))
            def _():
                along(o, t, -1).wait_send()

    @pl.loop(0, n_cp)
    def _(t):
        handed(t).wait_send()
        for i in range(1, chips):
            across(i, t).wait_send()
            arrived(i, t).wait_send()


def project_call(bounds, hidden, wq, wk, wv, inverse, n_cp, n_tp):
    rows, width = hidden.shape
    per = rows // BLOCK
    share = BLOCK // n_cp
    blocks = per * n_cp
    pieces = hidden.reshape(per, n_cp, share, width)
    bf, dma = jnp.bfloat16, pltpu.SemaphoreType.DMA
    vmem = pl.BlockSpec(memory_space=pltpu.VMEM)
    hbm = pl.BlockSpec(memory_space=pltpu.HBM)
    smem = pl.BlockSpec(memory_space=pltpu.SMEM)
    flops = 2 * rows * wq.shape[0] * (wq.shape[1] + 2 * HEAD_WIDTH)
    return pl.pallas_call(
        functools.partial(project_kernel, n_cp, n_tp),
        out_shape=(
            jax.ShapeDtypeStruct((rows, wq.shape[1]), bf),
            jax.ShapeDtypeStruct((blocks, n_cp, share, 2 * HEAD_WIDTH), bf),
        ),
        in_specs=[smem, hbm, hbm, hbm, hbm, vmem],
        out_specs=(vmem, vmem),
        scratch_shapes=[
            pltpu.VMEM((n_tp, blocks, share, width), bf),
            pltpu.VMEM(wq.shape, bf),
            pltpu.VMEM((wq.shape[0], 2 * HEAD_WIDTH), bf),
            pltpu.VMEM((rows, wq.shape[1]), jnp.float32),
            pltpu.VMEM((rows, 2 * HEAD_WIDTH), jnp.float32),
            pltpu.VMEM((blocks, share, 2 * HEAD_WIDTH), bf),
            pltpu.VMEM((blocks, n_cp, share, 2 * HEAD_WIDTH), bf),
            pltpu.VMEM((rows, HEAD_WIDTH), jnp.float32),
            pltpu.VMEM((rows, HEAD_WIDTH), jnp.float32),
            dma((3,)), dma, dma((n_cp,)), dma((n_cp,)),
            dma((n_tp, n_cp)), dma((n_tp, n_cp)), dma((n_tp, n_cp)),
            dma((n_cp // 2, n_cp)), dma((n_cp // 2, n_cp)),
            dma((n_cp // 2, n_cp)), dma((n_cp // 2, n_cp)),
        ],
        compiler_params=pltpu.CompilerParams(
            collective_id=1, has_side_effects=True, vmem_limit_bytes=48 << 20
        ),
        cost_estimate=pl.CostEstimate(flops=flops, bytes_accessed=12 << 20, transcendentals=0),
    )(bounds, pieces, wq, wk, wv, inverse)


def attend_kernel(bounds, owner, q_ref, kv_ref, out_ref, starts, tokens, where, *, heads, per):
    blocks, share = q_ref.shape[0], q_ref.shape[1]
    offset = lax.axis_index("cp") * share
    factor_of = math.log2(math.e) / math.sqrt(HEAD_WIDTH)
    keys = kv_ref.shape[0]
    window = min(WINDOW, keys)
    token_all, start_all = row_tokens(bounds, blocks, share, offset)
    tokens[...] = token_all
    starts[...] = start_all
    for d in range(blocks // per):
        where[blocks + d] = d * per
    for b in range(blocks):
        slot = where[blocks + owner[b]]
        where[b] = slot
        where[blocks + owner[b]] = slot + 1

    def stack(tile):
        return jnp.concatenate(
            [tile[:, h * HEAD_WIDTH : (h + 1) * HEAD_WIDTH] for h in range(heads)], axis=0
        )

    def scored(q, begin, stop, start, token):
        span = pl.ds(pl.multiple_of(begin, BLOCK), window)
        key = kv_ref[span, :HEAD_WIDTH]
        value = kv_ref[span, HEAD_WIDTH:]
        score = lax.dot_general(
            q, key, (((1,), (1,)), ((), ())), preferred_element_type=jnp.float32
        )
        index = begin + lax.broadcasted_iota(jnp.int32, score.shape, 1)
        allowed = (index >= start) & (index <= token)
        if stop is not None:
            allowed = allowed & (index < stop)
        return jnp.where(allowed, score, masked_score), value

    def one(b):
        q = stack(q_ref[b])
        start = jnp.tile(starts[b], (heads, 1))[:, :1]
        token = jnp.tile(tokens[b], (heads, 1))[:, :1]
        begin = jnp.maximum((b + 1) * BLOCK - window, 0)
        score, value = scored(q, begin, None, start, token)
        top = jnp.max(score, axis=1, keepdims=True)
        weight = jnp.exp2((score - top) * factor_of)
        total = jnp.sum(weight, axis=1, keepdims=True)
        out = dot(weight.astype(jnp.bfloat16), value)
        low = jnp.int32(0)
        for i in range(bounds.shape[0] - 1):
            low = jnp.where(b * BLOCK + offset >= bounds[i], bounds[i], low)

        def more(carry):
            stop, top, total, out = carry
            begin = jnp.maximum(stop - window, 0)
            score, value = scored(q, begin, stop, start, token)
            new_top = jnp.maximum(top, jnp.max(score, axis=1, keepdims=True))
            weight = jnp.exp2((score - new_top) * factor_of)
            factor = jnp.exp2((top - new_top) * factor_of)
            total = total * factor + jnp.sum(weight, axis=1, keepdims=True)
            out = out * factor + dot(weight.astype(jnp.bfloat16), value)
            return begin, new_top, total, out

        return low, more, (begin, top, total, out)

    group = 4

    @pl.loop(0, blocks // group)
    def _(g):
        firsts = [one(g * group + i) for i in range(group)]
        for i, (low, more, carry) in enumerate(firsts):
            _, _, total, out = lax.while_loop(lambda state: state[0] > low, more, carry)
            out = (out / total).astype(jnp.bfloat16)
            tile = jnp.concatenate(
                [out[h * share : (h + 1) * share] for h in range(heads)], axis=1
            )
            out_ref[where[g * group + i]] = tile


def attend_call(bounds, owner, q, kv, n_cp):
    rows, width = q.shape
    share = BLOCK // n_cp
    blocks = rows // share
    vmem = pl.BlockSpec(memory_space=pltpu.VMEM)
    smem = pl.BlockSpec(memory_space=pltpu.SMEM)
    return pl.pallas_call(
        functools.partial(attend_kernel, heads=width // HEAD_WIDTH, per=blocks // n_cp),
        out_shape=jax.ShapeDtypeStruct((blocks, share, width), jnp.bfloat16),
        in_specs=[smem, smem, vmem, vmem],
        out_specs=vmem,
        scratch_shapes=[
            pltpu.VMEM((blocks, share, HEAD_WIDTH), jnp.int32),
            pltpu.VMEM((blocks, share, HEAD_WIDTH), jnp.int32),
            pltpu.SMEM((blocks + n_cp,), jnp.int32),
        ],
        compiler_params=pltpu.CompilerParams(vmem_limit_bytes=32 << 20),
    )(bounds, owner, q.reshape(blocks, share, width), kv.reshape(-1, 2 * HEAD_WIDTH))


def output_kernel(
    n_cp, n_tp, heads, wo_hbm, out_ref,
    wo, part, from_left, from_right, to_right, to_left, done, landed,
    w_sem, r_send, l_send, r_recv, l_recv, a_send, a_recv,
):
    c, z = lax.axis_index("cp"), lax.axis_index("tp")
    per = out_ref.shape[0]
    share, width = heads.shape[1], out_ref.shape[3]

    def weight(o):
        cols = pl.ds(pl.multiple_of(o * width, width), width)
        return pltpu.make_async_copy(wo_hbm.at[:, cols], wo.at[o], w_sem.at[o])

    for s in range(n_tp - 1, -1, -1):
        @pl.when(z + s < n_tp)
        def _():
            weight(z + s).start()

        if s > 0:
            @pl.when(z - s >= 0)
            def _():
                weight(z - s).start()

    greet(n_cp, n_tp)

    def piece(t):
        return pl.ds(lax.rem(c + t, n_cp) * per, per)

    def rightward(o, t):
        return pltpu.make_async_remote_copy(
            src_ref=to_right.at[o, piece(t)], dst_ref=from_left.at[o, piece(t)],
            send_sem=r_send.at[o, t], recv_sem=r_recv.at[o, t],
            device_id={"tp": lax.rem(z + 1, n_tp)}, device_id_type=MESH,
        )

    def leftward(o, t):
        return pltpu.make_async_remote_copy(
            src_ref=to_left.at[o, piece(t)], dst_ref=from_right.at[o, piece(t)],
            send_sem=l_send.at[o, t], recv_sem=l_recv.at[o, t],
            device_id={"tp": lax.rem(z + n_tp - 1, n_tp)}, device_id_type=MESH,
        )

    def final(t):
        peer = lax.rem(c + t, n_cp)
        return pltpu.make_async_remote_copy(
            src_ref=done.at[piece(t)], dst_ref=landed.at[:, c],
            send_sem=a_send.at[t], recv_sem=a_recv.at[t],
            device_id={"cp": peer}, device_id_type=MESH,
        )

    def term(o):
        weight(o).wait()
        block = heads[...].reshape(-1, heads.shape[2])
        return dot(block, wo[o]).reshape(part.shape[1:])

    order = list(range(1, n_cp)) + [0]

    @pl.loop(0, n_tp - 1)
    def _(i):
        s = n_tp - 1 - i

        @pl.when(z + s < n_tp)
        def _():
            product = term(z + s)

            @pl.when(z == 0)
            def _():
                to_right[z + s] = product.astype(jnp.bfloat16)
                for t in order:
                    rightward(z + s, t).start()

            @pl.when(z > 0)
            def _():
                part[z + s] = product

        @pl.when(z - s >= 0)
        def _():
            product = term(z - s)

            @pl.when(z == n_tp - 1)
            def _():
                to_left[z - s] = product.astype(jnp.bfloat16)
                for t in order:
                    leftward(z - s, t).start()

            @pl.when(z < n_tp - 1)
            def _():
                part[z - s] = product

    part[z] = term(z)

    @pl.loop(0, n_tp - 1)
    def _(i):
        s = n_tp - 1 - i
        for t in order:
            @pl.when((z + s < n_tp) & (z > 0))
            def _():
                rightward(z + s, t).wait_recv()
                total = part[z + s, piece(t)] + from_left[z + s, piece(t)].astype(jnp.float32)
                to_right[z + s, piece(t)] = total.astype(jnp.bfloat16)
                rightward(z + s, t).start()

            @pl.when((z - s >= 0) & (z < n_tp - 1))
            def _():
                leftward(z - s, t).wait_recv()
                total = part[z - s, piece(t)] + from_right[z - s, piece(t)].astype(jnp.float32)
                to_left[z - s, piece(t)] = total.astype(jnp.bfloat16)
                leftward(z - s, t).start()

    for t in order:
        @pl.when(z > 0)
        def _():
            rightward(z, t).wait_recv()
            part[z, piece(t)] += from_left[z, piece(t)].astype(jnp.float32)

        @pl.when(z < n_tp - 1)
        def _():
            leftward(z, t).wait_recv()
            part[z, piece(t)] += from_right[z, piece(t)].astype(jnp.float32)

        done[piece(t)] = part[z, piece(t)].astype(jnp.bfloat16)
        if t > 0:
            final(t).start()

    for t in range(1, n_cp):
        final(t).wait_recv()
        source = lax.rem(c - t + n_cp, n_cp)
        out_ref[:, pl.ds(source, 1)] = landed[:, pl.ds(source, 1)]
    out_ref[:, pl.ds(c, 1)] = done[piece(0)][:, None]
    for t in range(1, n_cp):
        final(t).wait_send()
    for t in range(n_cp):
        for o in range(n_tp):
            @pl.when(o > z)
            def _():
                rightward(o, t).wait_send()

            @pl.when(o < z)
            def _():
                leftward(o, t).wait_send()


def output_call(heads, wo, n_cp, n_tp):
    blocks, share, depth = heads.shape
    width = wo.shape[1] // n_tp
    per = blocks // n_cp
    bf, dma = jnp.bfloat16, pltpu.SemaphoreType.DMA
    vmem = pl.BlockSpec(memory_space=pltpu.VMEM)
    slab = (n_tp, blocks, share, width)
    out = pl.pallas_call(
        functools.partial(output_kernel, n_cp, n_tp),
        out_shape=jax.ShapeDtypeStruct((per, n_cp, share, width), bf),
        in_specs=[vmem, pl.BlockSpec(memory_space=pltpu.HBM)],
        out_specs=vmem,
        scratch_shapes=[
            pltpu.VMEM((n_tp, depth, width), bf),
            pltpu.VMEM(slab, jnp.float32),
            pltpu.VMEM(slab, bf), pltpu.VMEM(slab, bf), pltpu.VMEM(slab, bf), pltpu.VMEM(slab, bf),
            pltpu.VMEM(slab[1:], bf),
            pltpu.VMEM((per, n_cp, share, width), bf),
            dma((n_tp,)), dma((n_tp, n_cp)), dma((n_tp, n_cp)), dma((n_tp, n_cp)), dma((n_tp, n_cp)),
            dma((n_cp,)), dma((n_cp,)),
        ],
        compiler_params=pltpu.CompilerParams(
            collective_id=2, has_side_effects=True, vmem_limit_bytes=48 << 20
        ),
        cost_estimate=pl.CostEstimate(
            flops=2 * blocks * share * depth * wo.shape[1], bytes_accessed=12 << 20, transcendentals=0
        ),
    )(heads, wo)
    return out.reshape(per * n_cp * share, width)


def local_fused(
    hidden, query_weight, key_matrix, value_matrix, output_weight, document_bounds, block_owner
):
    n_cp, n_tp = lax.axis_size("cp"), lax.axis_size("tp")
    inverse = jnp.tile(rope_inverse(HEAD_WIDTH), 2)[None, :]
    q, kv = project_call(
        document_bounds, hidden, query_weight, key_matrix, value_matrix, inverse, n_cp, n_tp
    )
    heads = attend_call(document_bounds, block_owner, q, kv, n_cp)
    return output_call(heads, output_weight, n_cp, n_tp)


def local_plain(
    hidden, query_weight, key_matrix, value_matrix, output_weight, document_bounds, block_owner
):
    cp_index = lax.axis_index("cp")
    row_count = hidden.shape[0]
    per_device = row_count // BLOCK
    block_order = owner_order(block_owner, per_device)
    own_blocks = lax.dynamic_slice_in_dim(block_order, cp_index * per_device, per_device, 0)
    new_tokens = (
        own_blocks[:, None] * BLOCK + jnp.arange(BLOCK, dtype=jnp.int32)[None, :]
    ).reshape(-1)
    kv_heads = key_matrix.shape[1] // HEAD_WIDTH
    moved = relayout(hidden, block_order)
    query_raw, key_raw, value_raw = project(moved, query_weight, key_matrix, value_matrix)
    queries = rotate(query_raw, new_tokens, document_bounds, HEAD_WIDTH)
    key_rows = rotate(key_raw, new_tokens, document_bounds, HEAD_WIDTH)
    value_rows = value_raw.astype(jnp.bfloat16)
    heads_out = attend(
        queries, new_tokens, key_rows, value_rows, new_tokens, document_bounds, HEAD_WIDTH, kv_heads
    )
    return output_rows(heads_out, output_weight)


def solution(mesh):
    shares = BLOCK // mesh.shape["cp"]
    local = local_fused if shares % 16 == 0 else local_plain
    placed = (P("cp", "tp"), P(None, "tp"), P(None, "tp"), P(None, "tp"), P("tp", None), P(), P())
    return jax.shard_map(
        local, mesh=mesh, in_specs=placed, out_specs=P("cp", "tp"), check_vma=False
    )
```
